32 devices in a mesh: dp: 4 (over x, y), tp: 8 (over z, core).
Axes of the slice: x: 2, y: 2, z: 4, core: 2. Of those that a mesh axis runs over, the one named last changes fastest.
Arguments:
- y_one: float32 [64, 128, 2048], P('dp', 'tp'), parts along dimension 0
- y_two: float32 [64, 128, 2048], P('dp', 'tp'), parts along dimension 0
- dy_one: float32 [64, 128, 2048], P('dp', 'tp'), parts along dimension 0
- dy_two: float32 [64, 128, 2048], P('dp', 'tp'), parts along dimension 0
- w_qkv: bfloat16 [1, 2048, 16, 3, 128], P(None, None, 'tp')
- w_out: bfloat16 [1, 16, 128, 2048], P(None, 'tp')
- w_up: bfloat16 [1, 2048, 8192], P(None, None, 'tp')
- w_down: bfloat16 [1, 8192, 2048], P(None, 'tp')
Outputs:
- output 1: float32 [64, 128, 2048], P('dp', 'tp'), parts along dimension 0
- output 2: float32 [64, 128, 2048], P('dp', 'tp'), parts along dimension 0
- output 3: float32 [64, 128, 2048], P('dp', 'tp'), parts along dimension 0
- output 4: float32 [64, 128, 2048], P('dp', 'tp'), parts along dimension 0
- output 5: float32 [4, 2048, 16, 3, 128], P('dp', None, 'tp'), parts along dimension 0
- output 6: float32 [4, 16, 128, 2048], P('dp', 'tp'), parts along dimension 0
- output 7: float32 [4, 2048, 8192], P('dp', None, 'tp'), parts along dimension 0
- output 8: float32 [4, 8192, 2048], P('dp', 'tp'), parts along dimension 0
There are 4 independent parts. The reference program is written for one: setup_inputs(seed, part) draws one part's arguments, and reference() takes and returns one part's arrays. A program takes and returns all parts, laid end to end along the dimension named above; an argument that names none is the same for every part.
All inputs are finite; a program needn't handle non-finite values.
Results may differ from the reference program's by a relative error of at most 0.00866442.
Values are sent between devices in bfloat16 or wider.
A program may use at most 1 GiB of HBM per device.

```python
import jax
import jax.numpy as jnp
from jax import lax

SEQ_COUNT = 16
SEQ_LEN = 128
HIDDEN = 2048
N_HEADS = 16
FFN_DIM = 8192
N_LAYERS = 1

HEAD_DIM = HIDDEN // N_HEADS
TOKENS = SEQ_COUNT * SEQ_LEN
STATE_SHAPE = (SEQ_COUNT, SEQ_LEN, HIDDEN)
RMS_EPS = 1e-6
ATTN_SCALE = HEAD_DIM ** -0.5
Q_GAIN = 2.5
OUT_GAIN = 0.6
DOWN_GAIN = 0.5


def setup_inputs(seed: int = 0, part: int = 0) -> dict:
    base_key = jax.random.key(seed)
    act_keys = jax.random.split(jax.random.fold_in(base_key, part), 4)
    w_keys = jax.random.split(jax.random.fold_in(base_key, 100003), 4)
    y_one = jax.random.normal(act_keys[0], STATE_SHAPE, jnp.float32)
    y_two = jax.random.normal(act_keys[1], STATE_SHAPE, jnp.float32)
    dy_one = jax.random.normal(act_keys[2], STATE_SHAPE, jnp.float32)
    dy_two = jax.random.normal(act_keys[3], STATE_SHAPE, jnp.float32)
    qkv_gain = jnp.array([Q_GAIN, 1.0, 1.0], jnp.float32).reshape(1, 1, 1, 3, 1)
    w_qkv = (jax.random.normal(w_keys[0], (N_LAYERS, HIDDEN, N_HEADS, 3, HEAD_DIM), jnp.float32) * qkv_gain * HIDDEN ** -0.5).astype(jnp.bfloat16)
    w_out = (jax.random.normal(w_keys[1], (N_LAYERS, N_HEADS, HEAD_DIM, HIDDEN), jnp.float32) * (OUT_GAIN * HIDDEN ** -0.5)).astype(jnp.bfloat16)
    w_up = (jax.random.normal(w_keys[2], (N_LAYERS, HIDDEN, FFN_DIM), jnp.float32) * HIDDEN ** -0.5).astype(jnp.bfloat16)
    w_down = (jax.random.normal(w_keys[3], (N_LAYERS, FFN_DIM, HIDDEN), jnp.float32) * (DOWN_GAIN * FFN_DIM ** -0.5)).astype(jnp.bfloat16)
    return {"y_one": y_one, "y_two": y_two, "dy_one": dy_one, "dy_two": dy_two, "w_qkv": w_qkv, "w_out": w_out, "w_up": w_up, "w_down": w_down}


def rms_norm(tensor):
    return tensor * lax.rsqrt(jnp.mean(tensor * tensor, axis=-1, keepdims=True) + RMS_EPS)


def rms_back(tensor, grad_in):
    inv_rms = lax.rsqrt(jnp.mean(tensor * tensor, axis=-1, keepdims=True) + RMS_EPS)
    return inv_rms * grad_in - tensor * (inv_rms * inv_rms * inv_rms) * jnp.mean(grad_in * tensor, axis=-1, keepdims=True)


def gelu_tanh(tensor):
    return jax.nn.gelu(tensor, approximate=True)


def mixed_dot(left, right):
    return jnp.dot(left, right, preferred_element_type=jnp.float32)


def as_wide(tensor):
    return tensor.astype(jnp.float32)


def attn_forward(qkv_seq):
    q_heads = as_wide(qkv_seq[0])
    k_heads = as_wide(qkv_seq[1])
    v_heads = as_wide(qkv_seq[2])
    scores = jnp.einsum("nqd,nkd->nqk", q_heads, k_heads) * ATTN_SCALE
    attn_prob = jax.nn.softmax(scores, axis=-1)
    context = jnp.einsum("nqk,nkd->nqd", as_wide(attn_prob.astype(jnp.bfloat16)), v_heads)
    return context.astype(jnp.bfloat16)


def attn_backward(operands):
    qkv_seq, d_context = operands
    q_heads = as_wide(qkv_seq[0])
    k_heads = as_wide(qkv_seq[1])
    v_heads = as_wide(qkv_seq[2])
    scores = jnp.einsum("nqd,nkd->nqk", q_heads, k_heads) * ATTN_SCALE
    attn_prob = jax.nn.softmax(scores, axis=-1)
    d_ctx = as_wide(d_context)
    d_prob = jnp.einsum("nqd,nkd->nqk", d_ctx, v_heads)
    d_value = jnp.einsum("nqk,nqd->nkd", as_wide(attn_prob.astype(jnp.bfloat16)), d_ctx)
    d_scores = attn_prob * (d_prob - jnp.sum(d_prob * attn_prob, axis=-1, keepdims=True)) * ATTN_SCALE
    d_scores = as_wide(d_scores.astype(jnp.bfloat16))
    d_query = jnp.einsum("nqk,nkd->nqd", d_scores, k_heads)
    d_key = jnp.einsum("nqk,nqd->nkd", d_scores, q_heads)
    return jnp.stack([d_query, d_key, d_value]).astype(jnp.bfloat16)


def block_backward(state_in, layer_weights):
    y_one, y_two, dy_one, dy_two = state_in
    w_qkv, w_out, w_up, w_down = layer_weights
    w_qkv_flat = w_qkv.reshape(HIDDEN, 3 * HIDDEN)
    w_out_flat = w_out.reshape(HIDDEN, HIDDEN)
    u_mlp = rms_norm(y_one).astype(jnp.bfloat16).reshape(TOKENS, HIDDEN)
    pre_act = mixed_dot(u_mlp, w_up)
    hidden, gelu_pull = jax.vjp(gelu_tanh, pre_act)
    hidden_b = hidden.astype(jnp.bfloat16)
    x_two = y_two - mixed_dot(hidden_b, w_down).reshape(STATE_SHAPE)
    cot_mlp = dy_two.astype(jnp.bfloat16).reshape(TOKENS, HIDDEN)
    dw_down = mixed_dot(hidden_b.T, cot_mlp)
    d_pre = gelu_pull(mixed_dot(cot_mlp, w_down.T))[0].astype(jnp.bfloat16)
    dw_up = mixed_dot(u_mlp.T, d_pre)
    dy_one = dy_one + rms_back(y_one, mixed_dot(d_pre, w_up.T).reshape(STATE_SHAPE))
    u_att = rms_norm(x_two).astype(jnp.bfloat16).reshape(TOKENS, HIDDEN)
    qkv_seqs = mixed_dot(u_att, w_qkv_flat).astype(jnp.bfloat16).reshape(SEQ_COUNT, SEQ_LEN, N_HEADS, 3, HEAD_DIM).transpose(0, 3, 2, 1, 4)
    context = lax.map(attn_forward, qkv_seqs)
    context_flat = context.transpose(0, 2, 1, 3).reshape(TOKENS, HIDDEN)
    x_one = y_one - mixed_dot(context_flat, w_out_flat).reshape(STATE_SHAPE)
    cot_att = dy_one.astype(jnp.bfloat16).reshape(TOKENS, HIDDEN)
    dw_out = mixed_dot(context_flat.T, cot_att)
    d_context = mixed_dot(cot_att, w_out_flat.T).astype(jnp.bfloat16).reshape(SEQ_COUNT, SEQ_LEN, N_HEADS, HEAD_DIM).transpose(0, 2, 1, 3)
    d_qkv = lax.map(attn_backward, (qkv_seqs, d_context))
    d_qkv_flat = d_qkv.transpose(0, 3, 2, 1, 4).reshape(TOKENS, 3 * HIDDEN)
    dw_qkv = mixed_dot(u_att.T, d_qkv_flat)
    dx_two = dy_two + rms_back(x_two, mixed_dot(d_qkv_flat, w_qkv_flat.T).reshape(STATE_SHAPE))
    grads = (dw_qkv.reshape(HIDDEN, N_HEADS, 3, HEAD_DIM), dw_out.reshape(N_HEADS, HEAD_DIM, HIDDEN), dw_up, dw_down)
    return (x_one, x_two, dy_one, dx_two), grads


def reference(y_one, y_two, dy_one, dy_two, w_qkv, w_out, w_up, w_down):
    final_state, grad_stack = lax.scan(block_backward, (y_one, y_two, dy_one, dy_two), (w_qkv, w_out, w_up, w_down), reverse=True)
    x_one, x_two, dx_one, dx_two = final_state
    dw_qkv, dw_out, dw_up, dw_down = grad_stack
    return (x_one, x_two, dx_one, dx_two, dw_qkv, dw_out, dw_up, dw_down)
```

```python
import jax
import jax.numpy as jnp
from jax import lax
from jax.experimental import pallas as pl
from jax.experimental.pallas import tpu as pltpu
from jax.sharding import PartitionSpec as P

RMS_EPS = 1e-6
N_CHIPS = 4

CORE_SWAP = [(i, i ^ 1) for i in range(2 * N_CHIPS)]
F32 = jnp.float32
MESH_ID = pl.DeviceIdType.MESH


def rms_norm(tensor):
    return tensor * lax.rsqrt(jnp.mean(tensor * tensor, axis=-1, keepdims=True) + RMS_EPS)


def rms_back(tensor, grad_in):
    inv_rms = lax.rsqrt(jnp.mean(tensor * tensor, axis=-1, keepdims=True) + RMS_EPS)
    return inv_rms * grad_in - tensor * (inv_rms * inv_rms * inv_rms) * jnp.mean(grad_in * tensor, axis=-1, keepdims=True)


def gelu_tanh(tensor):
    return jax.nn.gelu(tensor, approximate=True)


def gather_positions(tensor):
    return lax.all_gather(tensor, "tp", axis=1, tiled=True)


def scatter_positions(tensor):
    return lax.psum_scatter(tensor, "tp", scatter_dimension=1, tiled=True)


def dot(lhs, rhs, lhs_dim, rhs_dim):
    return lax.dot_general(lhs, rhs, (((lhs_dim,), (rhs_dim,)), ((), ())), preferred_element_type=F32)


def swap_core(tensor):
    return lax.ppermute(tensor, "tp", CORE_SWAP)


def mlp_kernel(u_ref, c_ref, w_up_ref, w_down_ref, g_ref, du_ref, up_all, down_all, u_all, c_all,
               u_chip, c_chip, up_tile, down_tile, tile_sem, pair_send, pair_recv, own_sem, send_sem, recv_sem):
    dp = lax.axis_index("dp")
    tp = lax.axis_index("tp")
    chip, core = tp // 2, tp % 2
    quarter_x = (dp + 2) % 4
    quarter_y = dp + 1 - 2 * (dp % 2)
    quarter_d = (quarter_x + 1) - 2 * (quarter_x % 2)
    at_x, at_y = (quarter_x, tp), (quarter_y, tp)
    at_up, at_down, at_core = (dp, tp + 2), (dp, tp - 2), (dp, tp + 1 - 2 * core)
    has_up, has_down = chip < N_CHIPS - 1, chip > 0
    own_refs, all_refs = (w_up_ref, w_down_ref), (up_all, down_all)
    tok_refs, tok_all = (u_ref, c_ref), (u_all, c_all)
    tile_rows = up_tile.shape[0]
    n_tok = u_ref.shape[0]

    barrier = pltpu.get_barrier_semaphore()
    for target in (at_x, at_y, at_core):
        pl.semaphore_signal(barrier, inc=1, device_id=target, device_id_type=MESH_ID)

    @pl.when(has_up)
    def _():
        pl.semaphore_signal(barrier, inc=1, device_id=at_up, device_id_type=MESH_ID)

    @pl.when(has_down)
    def _():
        pl.semaphore_signal(barrier, inc=1, device_id=at_down, device_id_type=MESH_ID)

    pl.semaphore_wait(barrier, 3 + has_up.astype(jnp.int32) + has_down.astype(jnp.int32))

    def send(kind, arr, src_chip, src, dst, target):
        recv_kind = 0 if kind == 1 else kind
        return pltpu.make_async_remote_copy(
            src_ref=src, dst_ref=dst, send_sem=send_sem.at[kind, arr, src_chip],
            recv_sem=recv_sem.at[recv_kind, arr, src_chip], device_id=target, device_id_type=MESH_ID)

    def line_copy(kind, arr, src_chip, from_own):
        dst = all_refs[arr].at[src_chip, dp]
        src = own_refs[arr].at[dp] if from_own else dst
        return send(kind, arr, src_chip, src, dst, at_up if kind == 0 else at_down)

    def token_copy(kind, i, src_chip, from_own):
        dst = tok_all[i].at[2 * src_chip + core]
        src = tok_refs[i] if from_own else dst
        return send(kind, 2 + i, src_chip, src, dst, (at_up, at_down, at_core)[kind])

    def plane_copy(kind, arr, src_chip):
        rows = all_refs[arr].shape[2]
        half = rows // 2
        if kind == 2:
            ref, target = all_refs[arr].at[src_chip, dp], at_x
        elif kind == 3:
            ref, target = all_refs[arr].at[src_chip, dp], at_y
        elif kind == 4:
            ref, target = all_refs[arr].at[src_chip, quarter_x, pl.ds(0, half)], at_y
        else:
            ref, target = all_refs[arr].at[src_chip, quarter_y, pl.ds(half, half)], at_x
        return send(kind, arr, src_chip, ref, ref, target)

    for arr in range(2):
        @pl.when(has_up)
        def _():
            line_copy(0, arr, chip, True).start()

        @pl.when(has_down)
        def _():
            line_copy(1, arr, chip, True).start()

    pair = []
    for i, (src, chip_ref) in enumerate(((u_ref, u_chip), (c_ref, c_chip))):
        copy = pltpu.make_async_remote_copy(
            src_ref=src, dst_ref=chip_ref.at[pl.ds(n_tok, n_tok)], send_sem=pair_send.at[i],
            recv_sem=pair_recv.at[i], device_id=at_core, device_id_type=MESH_ID)
        copy.start()
        keep = pltpu.make_async_copy(src, chip_ref.at[pl.ds(0, n_tok)], own_sem.at[i])
        keep.start()
        store = pltpu.make_async_copy(src, tok_all[i].at[tp], own_sem.at[2 + i])
        store.start()
        pair += [copy, keep, store]
    g_ref[...] = jnp.zeros_like(g_ref)
    du_ref[...] = jnp.zeros_like(du_ref)
    for copy in pair:
        copy.wait()

    def tile_step(src_chip, quarter, own):
        def load(refs, lead):
            return [pltpu.make_async_copy(ref.at[lead + (quarter, pl.ds(0, tile_rows))], buf, tile_sem.at[i])
                    for i, (ref, buf) in enumerate(zip(refs, (up_tile, down_tile)))]

        @pl.when(own)
        def _():
            for copy in load(own_refs, ()):
                copy.start()

        @pl.when(jnp.logical_not(own))
        def _():
            for copy in load(all_refs, (src_chip,)):
                copy.start()

        waits = load(own_refs, ())
        waits[0].wait()
        nt = (((1,), (1,)), ((), ()))
        pre = lax.dot_general(u_chip[...], up_tile[...], nt, preferred_element_type=F32)
        waits[1].wait()
        d_hid = lax.dot_general(c_chip[...], down_tile[...], nt, preferred_element_type=F32)
        hid, pull = jax.vjp(gelu_tanh, pre)
        g_ref[...] += jnp.dot(hid.astype(jnp.bfloat16), down_tile[...], preferred_element_type=F32)
        d_act = pull(d_hid)[0].astype(jnp.bfloat16)
        du_ref[...] += jnp.dot(d_act, up_tile[...], preferred_element_type=F32)

    def hop_chip(hop, side):
        other = chip - hop if side == 0 else chip + hop
        valid = other >= 0 if side == 0 else other < N_CHIPS
        return jnp.clip(other, 0, N_CHIPS - 1), jnp.logical_and(valid, jnp.logical_and(hop >= 1, hop <= N_CHIPS - 1))

    def step(it, carry):
        for arr in range(2):
            for side in range(2):
                other, valid = hop_chip(it, side)

                @pl.when(valid)
                def _():
                    line_copy(side, arr, other, False).wait_recv()
                    plane_copy(2, arr, other).start()
                    plane_copy(3, arr, other).start()

                @pl.when(jnp.logical_and(valid, has_up if side == 0 else has_down))
                def _():
                    line_copy(side, arr, other, False).start()

        @pl.when(it == 2)
        def _():
            for i in range(2):
                @pl.when(has_up)
                def _():
                    token_copy(0, i, chip, True).start()

                @pl.when(has_down)
                def _():
                    token_copy(1, i, chip, True).start()

                token_copy(2, i, chip, True).start()

        for i in range(2):
            for side in range(2):
                other, valid = hop_chip(it - 3, side)

                @pl.when(valid)
                def _():
                    token_copy(side, i, other, False).wait_recv()
                    token_copy(2, i, other, False).start()

                @pl.when(jnp.logical_and(valid, has_up if side == 0 else has_down))
                def _():
                    token_copy(side, i, other, False).start()

        for arr in range(2):
            for side in range(2):
                other, valid = hop_chip(it - 1, side)

                @pl.when(valid)
                def _():
                    plane_copy(2, arr, other).wait_recv()
                    plane_copy(4, arr, other).start()
                    plane_copy(3, arr, other).wait_recv()
                    plane_copy(5, arr, other).start()

        for side in range(2):
            other, valid = hop_chip(it - 2, side)

            @pl.when(valid)
            def _():
                for arr in range(2):
                    plane_copy(4, arr, other).wait_recv()
                    plane_copy(5, arr, other).wait_recv()

        def tiles(j, carry2):
            side = j // 4
            k = j % 4
            hop = jnp.where(it == 0, 0, jnp.where(k == 3, it - 2, it - 1))
            other = jnp.where(side == 0, chip - hop, chip + hop)
            in_line = jnp.logical_and(other >= 0, other < N_CHIPS)
            foreign = jnp.logical_and(in_line, jnp.logical_and(hop >= 1, hop <= N_CHIPS - 1))
            own = it == 0
            valid = jnp.where(own, side == 0, foreign)
            quarter = jnp.where(k == 0, dp, jnp.where(k == 1, quarter_x, jnp.where(k == 2, quarter_y, quarter_d)))

            @pl.when(valid)
            def _():
                tile_step(jnp.clip(other, 0, N_CHIPS - 1), quarter, own)

            return carry2

        return lax.fori_loop(0, 8, tiles, carry)

    lax.fori_loop(0, N_CHIPS + 3, step, 0)

    for arr in range(2):
        def drain(src_chip, carry):
            @pl.when(jnp.logical_and(has_up, src_chip <= chip))
            def _():
                line_copy(0, arr, src_chip, False).wait_send()

            @pl.when(jnp.logical_and(has_down, src_chip >= chip))
            def _():
                line_copy(1, arr, src_chip, False).wait_send()

            @pl.when(src_chip != chip)
            def _():
                for kind in (2, 3, 4, 5):
                    plane_copy(kind, arr, src_chip).wait_send()

            return carry

        lax.fori_loop(0, N_CHIPS, drain, 0)

    for i in range(2):
        def drain_tokens(src_chip, carry):
            @pl.when(jnp.logical_and(has_up, src_chip <= chip))
            def _():
                token_copy(0, i, src_chip, False).wait_send()

            @pl.when(jnp.logical_and(has_down, src_chip >= chip))
            def _():
                token_copy(1, i, src_chip, False).wait_send()

            token_copy(2, i, src_chip, False).wait()
            return carry

        lax.fori_loop(0, N_CHIPS, drain_tokens, 0)


def mlp_gather(u_own, c_own, up_rows, down_rows):
    n_tok, width = u_own.shape
    tile_rows = up_rows.shape[1]
    acc = jax.ShapeDtypeStruct((2 * n_tok, width), F32)
    gathered = [jax.ShapeDtypeStruct((N_CHIPS,) + r.shape, r.dtype) for r in (up_rows, down_rows)]
    gathered += [jax.ShapeDtypeStruct((2 * N_CHIPS,) + u_own.shape, u_own.dtype)] * 2
    vmem, anywhere = pl.BlockSpec(memory_space=pltpu.VMEM), pl.BlockSpec(memory_space=pl.ANY)
    n_col = N_CHIPS * 4 * tile_rows
    return pl.pallas_call(
        mlp_kernel,
        out_shape=[acc, acc] + gathered,
        in_specs=[vmem, vmem, anywhere, anywhere],
        out_specs=[vmem, vmem] + [anywhere] * 4,
        scratch_shapes=[
            pltpu.VMEM((2 * n_tok, width), jnp.bfloat16),
            pltpu.VMEM((2 * n_tok, width), jnp.bfloat16),
            pltpu.VMEM((tile_rows, width), jnp.bfloat16),
            pltpu.VMEM((tile_rows, width), jnp.bfloat16),
            pltpu.SemaphoreType.DMA((2,)),
            pltpu.SemaphoreType.DMA((2,)),
            pltpu.SemaphoreType.DMA((2,)),
            pltpu.SemaphoreType.DMA((4,)),
            pltpu.SemaphoreType.DMA((6, 4, N_CHIPS)),
            pltpu.SemaphoreType.DMA((6, 4, N_CHIPS)),
        ],
        compiler_params=pltpu.CompilerParams(collective_id=0, has_side_effects=True, vmem_limit_bytes=48 * 1024 * 1024),
        cost_estimate=pl.CostEstimate(flops=8 * 2 * n_tok * width * n_col * 4, bytes_accessed=64 * 1024 * 1024, transcendentals=0),
        name="mlp_gather",
    )(u_own, c_own, up_rows, down_rows)


def local_backward(y_one, y_two, dy_one, dy_two, w_qkv, w_out, w_up, w_down):
    attn_scale = w_qkv.shape[4] ** -0.5
    wq_layer, wo_layer, wu_layer, wd_layer = w_qkv[0], w_out[0], w_up[0], w_down[0]
    n_seq, n_pos, width = y_one.shape
    n_tok = n_seq * n_pos
    n_heads, head_dim = wo_layer.shape[0], wo_layer.shape[1]
    wo_flat = wo_layer.reshape(n_heads * head_dim, width)
    dp_idx = lax.axis_index("dp")
    tp_idx = lax.axis_index("tp")
    chip = tp_idx // 2
    f_loc = wu_layer.shape[1]
    f_quarter, o_quarter = f_loc // 4, n_heads * head_dim // 4

    u_own = rms_norm(y_one).astype(jnp.bfloat16)
    c_own = dy_two.astype(jnp.bfloat16)
    up_rows = wu_layer.T.reshape(4, f_quarter, width)
    down_rows = jnp.concatenate([wd_layer.reshape(4, f_quarter, width), wo_flat.reshape(4, o_quarter, width)], axis=1)
    g_sum, du_sum, _, down_all, u_mlp, cot_mlp = mlp_gather(u_own.reshape(n_tok, width), c_own.reshape(n_tok, width), up_rows, down_rows)
    g_own = g_sum[:n_tok] + swap_core(g_sum[n_tok:])
    du_own = du_sum[:n_tok] + swap_core(du_sum[n_tok:])
    core_out = lax.dynamic_update_index_in_dim(down_all[:, :, f_quarter:], wo_flat.reshape(4, o_quarter, width), chip, 0)
    core_out = core_out.reshape(N_CHIPS, n_heads * head_dim, width)
    other_out = swap_core(core_out)
    x_two = y_two - g_own.reshape(y_two.shape)
    dy_one = dy_one + rms_back(y_one, du_own.reshape(y_one.shape))

    u_mlp = u_mlp.reshape(2 * N_CHIPS * n_tok, width)
    cot_mlp = cot_mlp.reshape(2 * N_CHIPS * n_tok, width)
    hidden, gelu_pull = jax.vjp(gelu_tanh, dot(u_mlp, wu_layer, 1, 0))
    hidden_b = hidden.astype(jnp.bfloat16)
    grad_down = dot(hidden_b, cot_mlp, 0, 0)
    d_pre = gelu_pull(dot(cot_mlp, wd_layer, 1, 1))[0].astype(jnp.bfloat16)
    grad_up = dot(u_mlp, d_pre, 0, 0)

    u_att = gather_positions(rms_norm(x_two).astype(jnp.bfloat16))
    c_att_src, u_att = lax.optimization_barrier((dy_one.astype(jnp.bfloat16), u_att))
    cot_att = gather_positions(c_att_src)
    qkv_all = jnp.einsum("bsh,hnjd->jbnsd", u_att, wq_layer, preferred_element_type=F32).astype(jnp.bfloat16)
    q_heads, k_heads, v_heads = qkv_all[0], qkv_all[1], qkv_all[2]
    scores = jnp.einsum("bnqd,bnkd->bnqk", q_heads, k_heads, preferred_element_type=F32) * attn_scale
    attn_prob = jax.nn.softmax(scores, axis=-1)
    prob_b = attn_prob.astype(jnp.bfloat16)
    context = jnp.einsum("bnqk,bnkd->bnqd", prob_b, v_heads, preferred_element_type=F32).astype(jnp.bfloat16)

    ctx_send = context.transpose(2, 0, 1, 3).reshape(2 * N_CHIPS, n_pos * n_seq, n_heads * head_dim)
    ctx_recv = lax.all_to_all(ctx_send, "tp", 0, 0).reshape(N_CHIPS, 2, n_pos * n_seq, n_heads * head_dim)
    core = tp_idx % 2
    f_own = jnp.zeros((n_pos * n_seq, width), F32)
    for which, rows in ((core, core_out), (1 - core, other_out)):
        ctx_core = lax.dynamic_index_in_dim(ctx_recv, which, 1, keepdims=False)
        f_own = f_own + jnp.einsum("ztk,zkh->th", ctx_core, rows, preferred_element_type=F32)
    x_one = y_one - f_own.reshape(n_pos, n_seq, width).transpose(1, 0, 2)

    grad_out = jnp.einsum("bnqd,bqh->ndh", context, cot_att, preferred_element_type=F32)
    d_context = jnp.einsum("bqh,ndh->bnqd", cot_att, wo_layer, preferred_element_type=F32).astype(jnp.bfloat16)
    d_prob = jnp.einsum("bnqd,bnkd->bnqk", d_context, v_heads, preferred_element_type=F32)
    d_value = jnp.einsum("bnqk,bnqd->bnkd", prob_b, d_context, preferred_element_type=F32)
    d_scores = (attn_prob * (d_prob - jnp.sum(d_prob * attn_prob, axis=-1, keepdims=True)) * attn_scale).astype(jnp.bfloat16)
    d_query = jnp.einsum("bnqk,bnkd->bnqd", d_scores, k_heads, preferred_element_type=F32)
    d_key = jnp.einsum("bnqk,bnqd->bnkd", d_scores, q_heads, preferred_element_type=F32)
    d_qkv = jnp.stack([d_query.astype(jnp.bfloat16), d_key.astype(jnp.bfloat16), d_value.astype(jnp.bfloat16)])
    du_att = jnp.einsum("jbnsd,hnjd->bsh", d_qkv, wq_layer, preferred_element_type=F32)
    dx_two = dy_two + rms_back(x_two, scatter_positions(du_att))
    grad_qkv = jnp.einsum("bsh,jbnsd->hnjd", u_att, d_qkv, preferred_element_type=F32)

    return (x_one, x_two, dy_one, dx_two, grad_qkv[None], grad_out[None], grad_up[None], grad_down[None])


def solution(mesh):
    state_spec = P("dp", "tp", None)
    in_specs = (state_spec, state_spec, state_spec, state_spec, P(None, None, "tp", None, None), P(None, "tp", None, None), P(None, None, "tp"), P(None, "tp", None))
    out_specs = (state_spec, state_spec, state_spec, state_spec, P("dp", None, "tp", None, None), P("dp", "tp", None, None), P("dp", None, "tp"), P("dp", "tp", None))
    return jax.shard_map(local_backward, mesh=mesh, in_specs=in_specs, out_specs=out_specs, check_vma=False)
```

```python
import jax
import jax.numpy as jnp
from jax import lax
from jax.experimental import pallas as pl
from jax.experimental.pallas import tpu as pltpu
from jax.sharding import PartitionSpec as P

RMS_EPS = 1e-6
N_CHIPS = 4
N_WEIGHTS = 4

CORE_SWAP = [(i, i ^ 1) for i in range(2 * N_CHIPS)]
F32 = jnp.float32
MESH_ID = pl.DeviceIdType.MESH


def rms_norm(tensor):
    return tensor * lax.rsqrt(jnp.mean(tensor * tensor, axis=-1, keepdims=True) + RMS_EPS)


def rms_back(tensor, grad_in):
    inv_rms = lax.rsqrt(jnp.mean(tensor * tensor, axis=-1, keepdims=True) + RMS_EPS)
    return inv_rms * grad_in - tensor * (inv_rms * inv_rms * inv_rms) * jnp.mean(grad_in * tensor, axis=-1, keepdims=True)


def gelu_tanh(tensor):
    return jax.nn.gelu(tensor, approximate=True)


def gather_positions(tensor):
    return lax.all_gather(tensor, "tp", axis=1, tiled=True)


def dot(lhs, rhs, lhs_dim, rhs_dim):
    return lax.dot_general(lhs, rhs, (((lhs_dim,), (rhs_dim,)), ((), ())), preferred_element_type=F32)


def swap_core(tensor):
    return lax.ppermute(tensor, "tp", CORE_SWAP)


def mlp_kernel(u_ref, c_ref, w_up_ref, w_down_ref, w_out_ref, w_qkv_ref, g_ref, du_ref, up_all, down_all, out_all, qkv_all, u_all, c_all,
               u_chip, c_chip, up_tile, down_tile, tile_sem, pair_send, pair_recv, own_sem, send_sem, recv_sem):
    dp = lax.axis_index("dp")
    tp = lax.axis_index("tp")
    chip, core = tp // 2, tp % 2
    quarter_x = (dp + 2) % 4
    quarter_y = dp + 1 - 2 * (dp % 2)
    quarter_d = (quarter_x + 1) - 2 * (quarter_x % 2)
    at_x, at_y = (quarter_x, tp), (quarter_y, tp)
    at_up, at_down, at_core = (dp, tp + 2), (dp, tp - 2), (dp, tp + 1 - 2 * core)
    has_up, has_down = chip < N_CHIPS - 1, chip > 0
    own_refs, all_refs = (w_up_ref, w_down_ref, w_out_ref, w_qkv_ref), (up_all, down_all, out_all, qkv_all)
    tok_refs, tok_all = (u_ref, c_ref), (u_all, c_all)
    tile_rows = up_tile.shape[0]
    n_tok = u_ref.shape[0]

    barrier = pltpu.get_barrier_semaphore()
    for target in (at_x, at_y, at_core):
        pl.semaphore_signal(barrier, inc=1, device_id=target, device_id_type=MESH_ID)

    @pl.when(has_up)
    def _():
        pl.semaphore_signal(barrier, inc=1, device_id=at_up, device_id_type=MESH_ID)

    @pl.when(has_down)
    def _():
        pl.semaphore_signal(barrier, inc=1, device_id=at_down, device_id_type=MESH_ID)

    pl.semaphore_wait(barrier, 3 + has_up.astype(jnp.int32) + has_down.astype(jnp.int32))

    def send(kind, arr, src_chip, src, dst, target):
        recv_kind = 0 if kind == 1 else kind
        return pltpu.make_async_remote_copy(
            src_ref=src, dst_ref=dst, send_sem=send_sem.at[kind, arr, src_chip],
            recv_sem=recv_sem.at[recv_kind, arr, src_chip], device_id=target, device_id_type=MESH_ID)

    def line_copy(kind, arr, src_chip, from_own):
        dst = all_refs[arr].at[src_chip, dp]
        src = own_refs[arr].at[dp] if from_own else dst
        return send(kind, arr, src_chip, src, dst, at_up if kind == 0 else at_down)

    def token_copy(kind, i, src_chip, from_own):
        dst = tok_all[i].at[2 * src_chip + core]
        src = tok_refs[i] if from_own else dst
        return send(kind, N_WEIGHTS + i, src_chip, src, dst, (at_up, at_down, at_core)[kind])

    def plane_copy(kind, arr, src_chip):
        rows = all_refs[arr].shape[2]
        half = rows // 2
        if kind == 2:
            ref, target = all_refs[arr].at[src_chip, dp], at_x
        elif kind == 3:
            ref, target = all_refs[arr].at[src_chip, dp], at_y
        elif kind == 4:
            ref, target = all_refs[arr].at[src_chip, quarter_x, pl.ds(0, half)], at_y
        else:
            ref, target = all_refs[arr].at[src_chip, quarter_y, pl.ds(half, half)], at_x
        return send(kind, arr, src_chip, ref, ref, target)

    for arr in range(N_WEIGHTS):
        @pl.when(has_up)
        def _():
            line_copy(0, arr, chip, True).start()

        @pl.when(has_down)
        def _():
            line_copy(1, arr, chip, True).start()

    pair = []
    for i, (src, chip_ref) in enumerate(((u_ref, u_chip), (c_ref, c_chip))):
        copy = pltpu.make_async_remote_copy(
            src_ref=src, dst_ref=chip_ref.at[pl.ds(n_tok, n_tok)], send_sem=pair_send.at[i],
            recv_sem=pair_recv.at[i], device_id=at_core, device_id_type=MESH_ID)
        copy.start()
        keep = pltpu.make_async_copy(src, chip_ref.at[pl.ds(0, n_tok)], own_sem.at[i])
        keep.start()
        store = pltpu.make_async_copy(src, tok_all[i].at[tp], own_sem.at[2 + i])
        store.start()
        pair += [copy, keep, store]
    g_ref[...] = jnp.zeros_like(g_ref)
    du_ref[...] = jnp.zeros_like(du_ref)
    for copy in pair:
        copy.wait()

    def tile_step(src_chip, quarter, own):
        def load(refs, lead):
            return [pltpu.make_async_copy(ref.at[lead + (quarter, pl.ds(0, tile_rows))], buf, tile_sem.at[i])
                    for i, (ref, buf) in enumerate(zip(refs, (up_tile, down_tile)))]

        @pl.when(own)
        def _():
            for copy in load(own_refs, ()):
                copy.start()

        @pl.when(jnp.logical_not(own))
        def _():
            for copy in load(all_refs, (src_chip,)):
                copy.start()

        waits = load(own_refs, ())
        waits[0].wait()
        nt = (((1,), (1,)), ((), ()))
        pre = lax.dot_general(u_chip[...], up_tile[...], nt, preferred_element_type=F32)
        waits[1].wait()
        d_hid = lax.dot_general(c_chip[...], down_tile[...], nt, preferred_element_type=F32)
        hid, pull = jax.vjp(gelu_tanh, pre)
        g_ref[...] += jnp.dot(hid.astype(jnp.bfloat16), down_tile[...], preferred_element_type=F32)
        d_act = pull(d_hid)[0].astype(jnp.bfloat16)
        du_ref[...] += jnp.dot(d_act, up_tile[...], preferred_element_type=F32)

    def hop_chip(hop, side):
        other = chip - hop if side == 0 else chip + hop
        valid = other >= 0 if side == 0 else other < N_CHIPS
        return jnp.clip(other, 0, N_CHIPS - 1), jnp.logical_and(valid, jnp.logical_and(hop >= 1, hop <= N_CHIPS - 1))

    def token_hop(hop):
        for i in range(2):
            for side in range(2):
                other, valid = hop_chip(hop, side)

                @pl.when(valid)
                def _():
                    token_copy(side, i, other, False).wait_recv()
                    token_copy(2, i, other, False).start()

                @pl.when(jnp.logical_and(valid, has_up if side == 0 else has_down))
                def _():
                    token_copy(side, i, other, False).start()

    def step(it, carry):
        for arr in range(N_WEIGHTS):
            for side in range(2):
                other, valid = hop_chip(it, side)

                @pl.when(valid)
                def _():
                    line_copy(side, arr, other, False).wait_recv()
                    plane_copy(2, arr, other).start()
                    plane_copy(3, arr, other).start()

                @pl.when(jnp.logical_and(valid, has_up if side == 0 else has_down))
                def _():
                    line_copy(side, arr, other, False).start()

        @pl.when(it == 2)
        def _():
            for i in range(2):
                @pl.when(has_up)
                def _():
                    token_copy(0, i, chip, True).start()

                @pl.when(has_down)
                def _():
                    token_copy(1, i, chip, True).start()

                token_copy(2, i, chip, True).start()

        @pl.when(it < N_CHIPS + 1)
        def _():
            token_hop(it - 2)

        for arr in range(N_WEIGHTS):
            for side in range(2):
                other, valid = hop_chip(it - 1, side)

                @pl.when(valid)
                def _():
                    plane_copy(2, arr, other).wait_recv()
                    plane_copy(4, arr, other).start()
                    plane_copy(3, arr, other).wait_recv()
                    plane_copy(5, arr, other).start()

        for side in range(2):
            other, valid = hop_chip(it - 3, side)

            @pl.when(valid)
            def _():
                for arr in range(N_WEIGHTS):
                    plane_copy(4, arr, other).wait_recv()
                    plane_copy(5, arr, other).wait_recv()

        def tiles(j, carry2):
            side = j // 4
            k = j % 4
            hop = jnp.where(it == 0, 0, jnp.where(k == 3, it - 3, it - 1))
            other = jnp.where(side == 0, chip - hop, chip + hop)
            in_line = jnp.logical_and(other >= 0, other < N_CHIPS)
            foreign = jnp.logical_and(in_line, jnp.logical_and(hop >= 1, hop <= N_CHIPS - 1))
            own = it == 0
            valid = jnp.where(own, side == 0, foreign)
            quarter = jnp.where(k == 0, dp, jnp.where(k == 1, quarter_x, jnp.where(k == 2, quarter_y, quarter_d)))

            @pl.when(valid)
            def _():
                tile_step(jnp.clip(other, 0, N_CHIPS - 1), quarter, own)

            return carry2

        return lax.fori_loop(0, 8, tiles, carry)

    lax.fori_loop(0, N_CHIPS + 3, step, 0)
    token_hop(jnp.int32(N_CHIPS - 1))

    for arr in range(N_WEIGHTS):
        def drain(src_chip, carry):
            @pl.when(jnp.logical_and(has_up, src_chip <= chip))
            def _():
                line_copy(0, arr, src_chip, False).wait_send()

            @pl.when(jnp.logical_and(has_down, src_chip >= chip))
            def _():
                line_copy(1, arr, src_chip, False).wait_send()

            @pl.when(src_chip != chip)
            def _():
                for kind in (2, 3, 4, 5):
                    plane_copy(kind, arr, src_chip).wait_send()

            return carry

        lax.fori_loop(0, N_CHIPS, drain, 0)

    for i in range(2):
        def drain_tokens(src_chip, carry):
            @pl.when(jnp.logical_and(has_up, src_chip <= chip))
            def _():
                token_copy(0, i, src_chip, False).wait_send()

            @pl.when(jnp.logical_and(has_down, src_chip >= chip))
            def _():
                token_copy(1, i, src_chip, False).wait_send()

            token_copy(2, i, src_chip, False).wait()
            return carry

        lax.fori_loop(0, N_CHIPS, drain_tokens, 0)


def mlp_gather(u_own, c_own, *weight_rows):
    n_tok, width = u_own.shape
    tile_rows = weight_rows[0].shape[1]
    acc = jax.ShapeDtypeStruct((2 * n_tok, width), F32)
    gathered = [jax.ShapeDtypeStruct((N_CHIPS,) + r.shape, r.dtype) for r in weight_rows]
    gathered += [jax.ShapeDtypeStruct((2 * N_CHIPS,) + u_own.shape, u_own.dtype)] * 2
    vmem, anywhere = pl.BlockSpec(memory_space=pltpu.VMEM), pl.BlockSpec(memory_space=pl.ANY)
    n_col = N_CHIPS * 4 * tile_rows
    return pl.pallas_call(
        mlp_kernel,
        out_shape=[acc, acc] + gathered,
        in_specs=[vmem, vmem] + [anywhere] * N_WEIGHTS,
        out_specs=[vmem, vmem] + [anywhere] * (N_WEIGHTS + 2),
        scratch_shapes=[
            pltpu.VMEM((2 * n_tok, width), jnp.bfloat16),
            pltpu.VMEM((2 * n_tok, width), jnp.bfloat16),
            pltpu.VMEM((tile_rows, width), jnp.bfloat16),
            pltpu.VMEM((tile_rows, width), jnp.bfloat16),
            pltpu.SemaphoreType.DMA((2,)),
            pltpu.SemaphoreType.DMA((2,)),
            pltpu.SemaphoreType.DMA((2,)),
            pltpu.SemaphoreType.DMA((4,)),
            pltpu.SemaphoreType.DMA((6, N_WEIGHTS + 2, N_CHIPS)),
            pltpu.SemaphoreType.DMA((6, N_WEIGHTS + 2, N_CHIPS)),
        ],
        compiler_params=pltpu.CompilerParams(collective_id=0, has_side_effects=True, vmem_limit_bytes=48 * 1024 * 1024),
        cost_estimate=pl.CostEstimate(flops=8 * 2 * n_tok * width * n_col * 4, bytes_accessed=64 * 1024 * 1024, transcendentals=0),
        name="mlp_gather",
    )(u_own, c_own, *weight_rows)


def local_backward(y_one, y_two, dy_one, dy_two, w_qkv, w_out, w_up, w_down):
    attn_scale = w_qkv.shape[4] ** -0.5
    wq_layer, wo_layer, wu_layer, wd_layer = w_qkv[0], w_out[0], w_up[0], w_down[0]
    n_seq, n_pos, width = y_one.shape
    n_tok = n_seq * n_pos
    n_heads, head_dim = wo_layer.shape[0], wo_layer.shape[1]
    wo_flat = wo_layer.reshape(n_heads * head_dim, width)
    dp_idx = lax.axis_index("dp")
    tp_idx = lax.axis_index("tp")
    chip = tp_idx // 2
    f_loc = wu_layer.shape[1]
    f_quarter, o_quarter = f_loc // 4, n_heads * head_dim // 4

    u_own = rms_norm(y_one).astype(jnp.bfloat16)
    c_own = dy_two.astype(jnp.bfloat16)
    wqkv_rows = wq_layer.reshape(width, 3 * n_heads * head_dim).T
    own_rows = [w.reshape(4, w.shape[0] // 4, width) for w in (wu_layer.T, wd_layer, wo_flat, wqkv_rows)]
    g_sum, du_sum, _, _, out_all, qkv_rows_all, u_mlp, cot_mlp = mlp_gather(u_own.reshape(n_tok, width), c_own.reshape(n_tok, width), *own_rows)
    g_own = g_sum[:n_tok] + swap_core(g_sum[n_tok:])
    du_own = du_sum[:n_tok] + swap_core(du_sum[n_tok:])
    core_out = lax.dynamic_update_index_in_dim(out_all, own_rows[2], chip, 0).reshape(N_CHIPS, n_heads * head_dim, width)
    core_qkv = lax.dynamic_update_index_in_dim(qkv_rows_all, own_rows[3], chip, 0).reshape(N_CHIPS, 3 * n_heads * head_dim, width)
    other_out, other_qkv = swap_core(core_out), swap_core(core_qkv)
    x_two = y_two - g_own.reshape(y_two.shape)
    dy_one = dy_one + rms_back(y_one, du_own.reshape(y_one.shape))

    u_mlp = u_mlp.reshape(2 * N_CHIPS * n_tok, width)
    cot_mlp = cot_mlp.reshape(2 * N_CHIPS * n_tok, width)
    hidden, gelu_pull = jax.vjp(gelu_tanh, dot(u_mlp, wu_layer, 1, 0))
    hidden_b = hidden.astype(jnp.bfloat16)
    grad_down = dot(hidden_b, cot_mlp, 0, 0)
    d_pre = gelu_pull(dot(cot_mlp, wd_layer, 1, 1))[0].astype(jnp.bfloat16)
    grad_up = dot(u_mlp, d_pre, 0, 0)

    u_att = gather_positions(rms_norm(x_two).astype(jnp.bfloat16))
    half_seq = n_seq // 2
    halves = (slice(0, half_seq), slice(half_seq, n_seq))
    c_att = dy_one.astype(jnp.bfloat16)
    c_att, u_att, grad_up, grad_down = lax.optimization_barrier((c_att, u_att, grad_up, grad_down))
    cot_halves = [gather_positions(c_att[rows]) for rows in halves]
    qkv_all = jnp.einsum("bsh,hnjd->jbnsd", u_att, wq_layer, preferred_element_type=F32).astype(jnp.bfloat16)
    q_heads, k_heads, v_heads = qkv_all[0], qkv_all[1], qkv_all[2]
    scores = jnp.einsum("bnqd,bnkd->bnqk", q_heads, k_heads, preferred_element_type=F32) * attn_scale
    attn_prob = jax.nn.softmax(scores, axis=-1)
    prob_b = attn_prob.astype(jnp.bfloat16)
    context = jnp.einsum("bnqk,bnkd->bnqd", prob_b, v_heads, preferred_element_type=F32).astype(jnp.bfloat16)

    core = tp_idx % 2

    def sum_heads(by_pos, core_rows, other_rows):
        n_b, n_k = by_pos.shape[1], by_pos.shape[2]
        recv = lax.all_to_all(by_pos.reshape(2 * N_CHIPS, n_pos * n_b, n_k), "tp", 0, 0).reshape(N_CHIPS, 2, n_pos * n_b, n_k)
        total = jnp.zeros((n_pos * n_b, width), F32)
        for which, rows in ((core, core_rows), (1 - core, other_rows)):
            total = total + jnp.einsum("ztk,zkh->th", lax.dynamic_index_in_dim(recv, which, 1, keepdims=False), rows, preferred_element_type=F32)
        return total.reshape(n_pos, n_b, width).transpose(1, 0, 2)

    ctx_pos = context.transpose(2, 0, 1, 3).reshape(2 * N_CHIPS * n_pos, n_seq, n_heads * head_dim)
    x_one = y_one - sum_heads(ctx_pos, core_out, other_out)

    du_halves, d_qkv_halves = [], []
    for rows, cot_half in zip(halves, cot_halves):
        prob, prob_half = attn_prob[rows], prob_b[rows]
        d_context = jnp.einsum("bqh,ndh->bnqd", cot_half, wo_layer, preferred_element_type=F32).astype(jnp.bfloat16)
        d_prob = jnp.einsum("bnqd,bnkd->bnqk", d_context, v_heads[rows], preferred_element_type=F32)
        d_value = jnp.einsum("bnqk,bnqd->bnkd", prob_half, d_context, preferred_element_type=F32)
        d_scores = (prob * (d_prob - jnp.sum(d_prob * prob, axis=-1, keepdims=True)) * attn_scale).astype(jnp.bfloat16)
        d_query = jnp.einsum("bnqk,bnkd->bnqd", d_scores, k_heads[rows], preferred_element_type=F32)
        d_key = jnp.einsum("bnqk,bnqd->bnkd", d_scores, q_heads[rows], preferred_element_type=F32)
        d_qkv = jnp.stack([d_query.astype(jnp.bfloat16), d_key.astype(jnp.bfloat16), d_value.astype(jnp.bfloat16)])
        d_qkv_halves.append(d_qkv)
        d_pos = d_qkv.transpose(3, 1, 2, 0, 4).reshape(2 * N_CHIPS * n_pos, half_seq, 3 * n_heads * head_dim)
        du_halves.append(sum_heads(d_pos, core_qkv, other_qkv))
    dx_two = dy_two + rms_back(x_two, jnp.concatenate(du_halves, axis=0))
    d_qkv = jnp.concatenate(d_qkv_halves, axis=1)
    cot_att = jnp.concatenate(cot_halves, axis=0)
    grad_qkv = jnp.einsum("bsh,jbnsd->hnjd", u_att, d_qkv, preferred_element_type=F32)
    grad_out = jnp.einsum("bnqd,bqh->ndh", context, cot_att, preferred_element_type=F32)
    return (x_one, x_two, dy_one, dx_two, grad_qkv[None], grad_out[None], grad_up[None], grad_down[None])


def solution(mesh):
    state_spec = P("dp", "tp", None)
    in_specs = (state_spec, state_spec, state_spec, state_spec, P(None, None, "tp", None, None), P(None, "tp", None, None), P(None, None, "tp"), P(None, "tp", None))
    out_specs = (state_spec, state_spec, state_spec, state_spec, P("dp", None, "tp", None, None), P("dp", "tp", None, None), P("dp", None, "tp"), P("dp", "tp", None))
    return jax.shard_map(local_backward, mesh=mesh, in_specs=in_specs, out_specs=out_specs, check_vma=False)
```

```python
import jax
import jax.numpy as jnp
from jax import lax
from jax.experimental import pallas as pl
from jax.experimental.pallas import tpu as pltpu
from jax.sharding import PartitionSpec as P

RMS_EPS = 1e-6
N_CHIPS = 4
N_WEIGHTS = 4

CORE_SWAP = [(i, i ^ 1) for i in range(2 * N_CHIPS)]
F32 = jnp.float32
MESH_ID = pl.DeviceIdType.MESH


def rms_norm(tensor):
    return tensor * lax.rsqrt(jnp.mean(tensor * tensor, axis=-1, keepdims=True) + RMS_EPS)


def rms_back(tensor, grad_in):
    inv_rms = lax.rsqrt(jnp.mean(tensor * tensor, axis=-1, keepdims=True) + RMS_EPS)
    return inv_rms * grad_in - tensor * (inv_rms * inv_rms * inv_rms) * jnp.mean(grad_in * tensor, axis=-1, keepdims=True)


def gelu_tanh(tensor):
    return jax.nn.gelu(tensor, approximate=True)


def gather_positions(tensor):
    return lax.all_gather(tensor, "tp", axis=1, tiled=True)


def dot(lhs, rhs, lhs_dim, rhs_dim):
    return lax.dot_general(lhs, rhs, (((lhs_dim,), (rhs_dim,)), ((), ())), preferred_element_type=F32)


def swap_core(tensor):
    return lax.ppermute(tensor, "tp", CORE_SWAP)


def mlp_kernel(u_ref, c_ref, w_up_ref, w_down_ref, w_out_ref, w_qkv_ref, g_ref, du_ref, up_all, down_all, out_all, qkv_all, u_all, c_all,
               u_chip, c_chip, up_tile, down_tile, tile_sem, pair_send, pair_recv, own_sem, send_sem, recv_sem):
    dp = lax.axis_index("dp")
    tp = lax.axis_index("tp")
    chip, core = tp // 2, tp % 2
    quarter_x = (dp + 2) % 4
    quarter_y = dp + 1 - 2 * (dp % 2)
    quarter_d = (quarter_x + 1) - 2 * (quarter_x % 2)
    at_x, at_y = (quarter_x, tp), (quarter_y, tp)
    at_up, at_down, at_core = (dp, tp + 2), (dp, tp - 2), (dp, tp + 1 - 2 * core)
    has_up, has_down = chip < N_CHIPS - 1, chip > 0
    own_refs, all_refs = (w_up_ref, w_down_ref, w_out_ref, w_qkv_ref), (up_all, down_all, out_all, qkv_all)
    tok_refs, tok_all = (u_ref, c_ref), (u_all, c_all)
    tile_rows = up_tile.shape[0]
    n_tok = u_ref.shape[0]

    barrier = pltpu.get_barrier_semaphore()
    for target in (at_x, at_y, at_core):
        pl.semaphore_signal(barrier, inc=1, device_id=target, device_id_type=MESH_ID)

    @pl.when(has_up)
    def _():
        pl.semaphore_signal(barrier, inc=1, device_id=at_up, device_id_type=MESH_ID)

    @pl.when(has_down)
    def _():
        pl.semaphore_signal(barrier, inc=1, device_id=at_down, device_id_type=MESH_ID)

    pl.semaphore_wait(barrier, 3 + has_up.astype(jnp.int32) + has_down.astype(jnp.int32))

    def send(kind, arr, src_chip, src, dst, target):
        recv_kind = 0 if kind == 1 else kind
        return pltpu.make_async_remote_copy(
            src_ref=src, dst_ref=dst, send_sem=send_sem.at[kind, arr, src_chip],
            recv_sem=recv_sem.at[recv_kind, arr, src_chip], device_id=target, device_id_type=MESH_ID)

    def line_copy(kind, arr, src_chip, from_own):
        dst = all_refs[arr].at[src_chip, dp]
        src = own_refs[arr].at[dp if own_refs[arr].shape[0] == N_CHIPS else 0] if from_own else dst
        return send(kind, arr, src_chip, src, dst, at_up if kind == 0 else at_down)

    def token_copy(kind, i, src_chip, from_own):
        dst = tok_all[i].at[2 * src_chip + core]
        src = tok_refs[i] if from_own else dst
        return send(kind, N_WEIGHTS + i, src_chip, src, dst, (at_up, at_down, at_core)[kind])

    def plane_copy(kind, arr, src_chip):
        rows = all_refs[arr].shape[2]
        half = rows // 2
        if kind == 2:
            ref, target = all_refs[arr].at[src_chip, dp], at_x
        elif kind == 3:
            ref, target = all_refs[arr].at[src_chip, dp], at_y
        elif kind == 4:
            ref, target = all_refs[arr].at[src_chip, quarter_x, pl.ds(0, half)], at_y
        else:
            ref, target = all_refs[arr].at[src_chip, quarter_y, pl.ds(half, half)], at_x
        return send(kind, arr, src_chip, ref, ref, target)

    for arr in range(N_WEIGHTS):
        @pl.when(has_up)
        def _():
            line_copy(0, arr, chip, True).start()

        @pl.when(has_down)
        def _():
            line_copy(1, arr, chip, True).start()

    pair = []
    for i, (src, chip_ref) in enumerate(((u_ref, u_chip), (c_ref, c_chip))):
        copy = pltpu.make_async_remote_copy(
            src_ref=src, dst_ref=chip_ref.at[pl.ds(n_tok, n_tok)], send_sem=pair_send.at[i],
            recv_sem=pair_recv.at[i], device_id=at_core, device_id_type=MESH_ID)
        copy.start()
        keep = pltpu.make_async_copy(src, chip_ref.at[pl.ds(0, n_tok)], own_sem.at[i])
        keep.start()
        store = pltpu.make_async_copy(src, tok_all[i].at[tp], own_sem.at[2 + i])
        store.start()
        pair += [copy, keep, store]
    g_ref[...] = jnp.zeros_like(g_ref)
    du_ref[...] = jnp.zeros_like(du_ref)
    for copy in pair:
        copy.wait()

    def tile_step(src_chip, quarter, own):
        def load(refs, lead):
            return [pltpu.make_async_copy(ref.at[lead + (quarter, pl.ds(0, tile_rows))], buf, tile_sem.at[i])
                    for i, (ref, buf) in enumerate(zip(refs, (up_tile, down_tile)))]

        @pl.when(own)
        def _():
            for copy in load(own_refs, ()):
                copy.start()

        @pl.when(jnp.logical_not(own))
        def _():
            for copy in load(all_refs, (src_chip,)):
                copy.start()

        waits = load(own_refs, ())
        waits[0].wait()
        nt = (((1,), (1,)), ((), ()))
        pre = lax.dot_general(u_chip[...], up_tile[...], nt, preferred_element_type=F32)
        waits[1].wait()
        d_hid = lax.dot_general(c_chip[...], down_tile[...], nt, preferred_element_type=F32)
        hid, pull = jax.vjp(gelu_tanh, pre)
        g_ref[...] += jnp.dot(hid.astype(jnp.bfloat16), down_tile[...], preferred_element_type=F32)
        d_act = pull(d_hid)[0].astype(jnp.bfloat16)
        du_ref[...] += jnp.dot(d_act, up_tile[...], preferred_element_type=F32)

    def hop_chip(hop, side):
        other = chip - hop if side == 0 else chip + hop
        valid = other >= 0 if side == 0 else other < N_CHIPS
        return jnp.clip(other, 0, N_CHIPS - 1), jnp.logical_and(valid, jnp.logical_and(hop >= 1, hop <= N_CHIPS - 1))

    def token_hop(hop):
        for i in range(2):
            for side in range(2):
                other, valid = hop_chip(hop, side)

                @pl.when(valid)
                def _():
                    token_copy(side, i, other, False).wait_recv()
                    token_copy(2, i, other, False).start()

                @pl.when(jnp.logical_and(valid, has_up if side == 0 else has_down))
                def _():
                    token_copy(side, i, other, False).start()

    def step(it, carry):
        for arr in range(N_WEIGHTS):
            for side in range(2):
                other, valid = hop_chip(it, side)

                @pl.when(valid)
                def _():
                    line_copy(side, arr, other, False).wait_recv()
                    plane_copy(2, arr, other).start()
                    plane_copy(3, arr, other).start()

                @pl.when(jnp.logical_and(valid, has_up if side == 0 else has_down))
                def _():
                    line_copy(side, arr, other, False).start()

        @pl.when(it == 2)
        def _():
            for i in range(2):
                @pl.when(has_up)
                def _():
                    token_copy(0, i, chip, True).start()

                @pl.when(has_down)
                def _():
                    token_copy(1, i, chip, True).start()

                token_copy(2, i, chip, True).start()

        @pl.when(it < N_CHIPS + 1)
        def _():
            token_hop(it - 2)

        for arr in range(N_WEIGHTS):
            for side in range(2):
                other, valid = hop_chip(it - 1, side)

                @pl.when(valid)
                def _():
                    plane_copy(2, arr, other).wait_recv()
                    plane_copy(4, arr, other).start()
                    plane_copy(3, arr, other).wait_recv()
                    plane_copy(5, arr, other).start()

        for side in range(2):
            other, valid = hop_chip(it - 3, side)

            @pl.when(valid)
            def _():
                for arr in range(N_WEIGHTS):
                    plane_copy(4, arr, other).wait_recv()
                    plane_copy(5, arr, other).wait_recv()

        def tiles(j, carry2):
            side = j // 4
            k = j % 4
            hop = jnp.where(it == 0, 0, jnp.where(k == 3, it - 3, it - 1))
            other = jnp.where(side == 0, chip - hop, chip + hop)
            in_line = jnp.logical_and(other >= 0, other < N_CHIPS)
            foreign = jnp.logical_and(in_line, jnp.logical_and(hop >= 1, hop <= N_CHIPS - 1))
            own = it == 0
            valid = jnp.where(own, side == 0, foreign)
            quarter = jnp.where(k == 0, dp, jnp.where(k == 1, quarter_x, jnp.where(k == 2, quarter_y, quarter_d)))

            @pl.when(valid)
            def _():
                tile_step(jnp.clip(other, 0, N_CHIPS - 1), quarter, own)

            return carry2

        return lax.fori_loop(0, 8, tiles, carry)

    lax.fori_loop(0, N_CHIPS + 3, step, 0)
    token_hop(jnp.int32(N_CHIPS - 1))

    for arr in range(N_WEIGHTS):
        def drain(src_chip, carry):
            @pl.when(jnp.logical_and(has_up, src_chip <= chip))
            def _():
                line_copy(0, arr, src_chip, False).wait_send()

            @pl.when(jnp.logical_and(has_down, src_chip >= chip))
            def _():
                line_copy(1, arr, src_chip, False).wait_send()

            @pl.when(src_chip != chip)
            def _():
                for kind in (2, 3, 4, 5):
                    plane_copy(kind, arr, src_chip).wait_send()

            return carry

        lax.fori_loop(0, N_CHIPS, drain, 0)

    for i in range(2):
        def drain_tokens(src_chip, carry):
            @pl.when(jnp.logical_and(has_up, src_chip <= chip))
            def _():
                token_copy(0, i, src_chip, False).wait_send()

            @pl.when(jnp.logical_and(has_down, src_chip >= chip))
            def _():
                token_copy(1, i, src_chip, False).wait_send()

            token_copy(2, i, src_chip, False).wait()
            return carry

        lax.fori_loop(0, N_CHIPS, drain_tokens, 0)


def mlp_gather(u_own, c_own, *weight_rows):
    n_tok, width = u_own.shape
    tile_rows = weight_rows[0].shape[1]
    acc = jax.ShapeDtypeStruct((2 * n_tok, width), F32)
    gathered = [jax.ShapeDtypeStruct((N_CHIPS, 4) + r.shape[1:], r.dtype) for r in weight_rows]
    gathered += [jax.ShapeDtypeStruct((2 * N_CHIPS,) + u_own.shape, u_own.dtype)] * 2
    vmem, anywhere = pl.BlockSpec(memory_space=pltpu.VMEM), pl.BlockSpec(memory_space=pl.ANY)
    n_col = N_CHIPS * 4 * tile_rows
    return pl.pallas_call(
        mlp_kernel,
        out_shape=[acc, acc] + gathered,
        in_specs=[vmem, vmem] + [anywhere] * N_WEIGHTS,
        out_specs=[vmem, vmem] + [anywhere] * (N_WEIGHTS + 2),
        scratch_shapes=[
            pltpu.VMEM((2 * n_tok, width), jnp.bfloat16),
            pltpu.VMEM((2 * n_tok, width), jnp.bfloat16),
            pltpu.VMEM((tile_rows, width), jnp.bfloat16),
            pltpu.VMEM((tile_rows, width), jnp.bfloat16),
            pltpu.SemaphoreType.DMA((2,)),
            pltpu.SemaphoreType.DMA((2,)),
            pltpu.SemaphoreType.DMA((2,)),
            pltpu.SemaphoreType.DMA((4,)),
            pltpu.SemaphoreType.DMA((6, N_WEIGHTS + 2, N_CHIPS)),
            pltpu.SemaphoreType.DMA((6, N_WEIGHTS + 2, N_CHIPS)),
        ],
        compiler_params=pltpu.CompilerParams(collective_id=0, has_side_effects=True, vmem_limit_bytes=48 * 1024 * 1024),
        cost_estimate=pl.CostEstimate(flops=8 * 2 * n_tok * width * n_col * 4, bytes_accessed=64 * 1024 * 1024, transcendentals=0),
        name="mlp_gather",
    )(u_own, c_own, *weight_rows)


def local_backward(y_one, y_two, dy_one, dy_two, w_qkv, w_out, w_up, w_down):
    attn_scale = w_qkv.shape[4] ** -0.5
    wq_layer, wo_layer, wu_layer, wd_layer = w_qkv[0], w_out[0], w_up[0], w_down[0]
    n_seq, n_pos, width = y_one.shape
    n_tok = n_seq * n_pos
    n_heads, head_dim = wo_layer.shape[0], wo_layer.shape[1]
    wo_flat = wo_layer.reshape(n_heads * head_dim, width)
    dp_idx = lax.axis_index("dp")
    tp_idx = lax.axis_index("tp")
    chip = tp_idx // 2
    f_loc = wu_layer.shape[1]
    f_quarter, o_quarter = f_loc // 4, n_heads * head_dim // 4

    u_own = rms_norm(y_one).astype(jnp.bfloat16)
    c_own = dy_two.astype(jnp.bfloat16)
    n_qkv = 3 * n_heads * head_dim
    own_rows = [w.reshape(4, w.shape[0] // 4, width) for w in (wu_layer.T, wd_layer, wo_flat)]
    own_rows.append(lax.dynamic_slice_in_dim(wq_layer, dp_idx * (width // 4), width // 4, 0).reshape(1, width // 4, n_qkv))
    g_sum, du_sum, _, _, out_all, qkv_rows_all, u_mlp, cot_mlp = mlp_gather(u_own.reshape(n_tok, width), c_own.reshape(n_tok, width), *own_rows)
    g_own = g_sum[:n_tok] + swap_core(g_sum[n_tok:])
    du_own = du_sum[:n_tok] + swap_core(du_sum[n_tok:])
    core_out = lax.dynamic_update_index_in_dim(out_all, own_rows[2], chip, 0).reshape(N_CHIPS, n_heads * head_dim, width)
    core_qkv = lax.dynamic_update_index_in_dim(qkv_rows_all.reshape(N_CHIPS, width, n_qkv), wq_layer.reshape(width, n_qkv), chip, 0)
    other_out, other_qkv = swap_core(core_out), swap_core(core_qkv)
    x_two = y_two - g_own.reshape(y_two.shape)
    dy_one = dy_one + rms_back(y_one, du_own.reshape(y_one.shape))

    u_mlp = u_mlp.reshape(2 * N_CHIPS * n_tok, width)
    cot_mlp = cot_mlp.reshape(2 * N_CHIPS * n_tok, width)
    hidden, gelu_pull = jax.vjp(gelu_tanh, dot(u_mlp, wu_layer, 1, 0))
    hidden_b = hidden.astype(jnp.bfloat16)
    grad_down = dot(hidden_b, cot_mlp, 0, 0)
    d_pre = gelu_pull(dot(cot_mlp, wd_layer, 1, 1))[0].astype(jnp.bfloat16)
    grad_up = dot(u_mlp, d_pre, 0, 0)

    u_att = gather_positions(rms_norm(x_two).astype(jnp.bfloat16))
    half_seq = n_seq // 2
    halves = (slice(0, half_seq), slice(half_seq, n_seq))
    c_att = dy_one.astype(jnp.bfloat16)
    c_att, u_att, grad_up, grad_down = lax.optimization_barrier((c_att, u_att, grad_up, grad_down))
    cot_halves = [gather_positions(c_att[rows]) for rows in halves]
    qkv_all = jnp.einsum("bsh,hnjd->jbnsd", u_att, wq_layer, preferred_element_type=F32).astype(jnp.bfloat16)
    q_heads, k_heads, v_heads = qkv_all[0], qkv_all[1], qkv_all[2]
    scores = jnp.einsum("bnqd,bnkd->bnqk", q_heads, k_heads, preferred_element_type=F32) * attn_scale
    attn_prob = jax.nn.softmax(scores, axis=-1)
    prob_b = attn_prob.astype(jnp.bfloat16)
    context = jnp.einsum("bnqk,bnkd->bnqd", prob_b, v_heads, preferred_element_type=F32).astype(jnp.bfloat16)

    core = tp_idx % 2

    def to_positions(by_pos):
        n_b, n_k = by_pos.shape[1], by_pos.shape[2]
        return lax.all_to_all(by_pos.reshape(2 * N_CHIPS, n_pos * n_b, n_k), "tp", 0, 0).reshape(N_CHIPS, 2, n_pos * n_b, n_k)

    def sum_heads(recv, core_rows, other_rows, form):
        total = jnp.zeros((recv.shape[2], width), F32)
        for which, rows in ((core, core_rows), (1 - core, other_rows)):
            total = total + jnp.einsum(form, lax.dynamic_index_in_dim(recv, which, 1, keepdims=False), rows, preferred_element_type=F32)
        return total.reshape(n_pos, -1, width).transpose(1, 0, 2)

    ctx_pos = context.transpose(2, 0, 1, 3).reshape(2 * N_CHIPS * n_pos, n_seq, n_heads * head_dim)
    ctx_recv = to_positions(ctx_pos)

    du_halves, grad_qkv, grad_out = [], None, None
    for half_idx, rows in enumerate(halves):
        cot_half = cot_halves[half_idx]
        prob, prob_half = attn_prob[rows], prob_b[rows]
        d_context = jnp.einsum("bqh,ndh->bnqd", cot_half, wo_layer, preferred_element_type=F32).astype(jnp.bfloat16)
        d_prob = jnp.einsum("bnqd,bnkd->bnqk", d_context, v_heads[rows], preferred_element_type=F32)
        d_value = jnp.einsum("bnqk,bnqd->bnkd", prob_half, d_context, preferred_element_type=F32)
        d_scores = (prob * (d_prob - jnp.sum(d_prob * prob, axis=-1, keepdims=True)) * attn_scale).astype(jnp.bfloat16)
        d_query = jnp.einsum("bnqk,bnkd->bnqd", d_scores, k_heads[rows], preferred_element_type=F32)
        d_key = jnp.einsum("bnqk,bnqd->bnkd", d_scores, q_heads[rows], preferred_element_type=F32)
        d_qkv = jnp.stack([d_query.astype(jnp.bfloat16), d_key.astype(jnp.bfloat16), d_value.astype(jnp.bfloat16)])
        d_pos = d_qkv.transpose(3, 1, 2, 0, 4).reshape(2 * N_CHIPS * n_pos, half_seq, n_qkv)
        if half_idx == 0:
            d_pos, ctx_recv = lax.optimization_barrier((d_pos, ctx_recv))
            x_one = y_one - sum_heads(ctx_recv, core_out, other_out, "ztk,zkh->th")
        du_halves.append(sum_heads(to_positions(d_pos), core_qkv, other_qkv, "ztk,zhk->th"))
        grad_qkv_half = jnp.einsum("bsh,jbnsd->hnjd", u_att[rows], d_qkv, preferred_element_type=F32)
        grad_out_half = jnp.einsum("bnqd,bqh->ndh", context[rows], cot_half, preferred_element_type=F32)
        if half_idx == 0:
            grad_qkv, grad_out = grad_qkv_half, grad_out_half
            held = (cot_halves[1], grad_qkv, grad_out, du_halves[0], x_one)
            cot_halves[1], grad_qkv, grad_out, du_halves[0], x_one = lax.optimization_barrier(held)
        else:
            grad_qkv, grad_out = grad_qkv + grad_qkv_half, grad_out + grad_out_half
    dx_two = dy_two + rms_back(x_two, jnp.concatenate(du_halves, axis=0))
    return (x_one, x_two, dy_one, dx_two, grad_qkv[None], grad_out[None], grad_up[None], grad_down[None])


def solution(mesh):
    state_spec = P("dp", "tp", None)
    in_specs = (state_spec, state_spec, state_spec, state_spec, P(None, None, "tp", None, None), P(None, "tp", None, None), P(None, None, "tp"), P(None, "tp", None))
    out_specs = (state_spec, state_spec, state_spec, state_spec, P("dp", None, "tp", None, None), P("dp", "tp", None, None), P("dp", None, "tp"), P("dp", "tp", None))
    return jax.shard_map(local_backward, mesh=mesh, in_specs=in_specs, out_specs=out_specs, check_vma=False)
```

```python
import jax
import jax.numpy as jnp
from jax import lax
from jax.experimental import pallas as pl
from jax.experimental.pallas import tpu as pltpu
from jax.sharding import PartitionSpec as P

RMS_EPS = 1e-6
N_CHIPS = 4
N_WEIGHTS = 4

CORE_SWAP = [(i, i ^ 1) for i in range(2 * N_CHIPS)]
F32 = jnp.float32
MESH_ID = pl.DeviceIdType.MESH


def rms_norm(tensor):
    return tensor * lax.rsqrt(jnp.mean(tensor * tensor, axis=-1, keepdims=True) + RMS_EPS)


def rms_back(tensor, grad_in):
    inv_rms = lax.rsqrt(jnp.mean(tensor * tensor, axis=-1, keepdims=True) + RMS_EPS)
    return inv_rms * grad_in - tensor * (inv_rms * inv_rms * inv_rms) * jnp.mean(grad_in * tensor, axis=-1, keepdims=True)


def gelu_tanh(tensor):
    return jax.nn.gelu(tensor, approximate=True)


def gather_positions(tensor):
    return lax.all_gather(tensor, "tp", axis=1, tiled=True)


def dot(lhs, rhs, lhs_dim, rhs_dim):
    return lax.dot_general(lhs, rhs, (((lhs_dim,), (rhs_dim,)), ((), ())), preferred_element_type=F32)


def swap_core(tensor):
    return lax.ppermute(tensor, "tp", CORE_SWAP)


def mlp_kernel(u_ref, c_ref, w_up_ref, w_down_ref, w_out_ref, w_qkv_ref, g_ref, du_ref, up_all, down_all, out_all, qkv_all, u_all, c_all,
               u_chip, c_chip, up_tile, down_tile, tile_sem, pair_send, pair_recv, own_sem, send_sem, recv_sem):
    dp = lax.axis_index("dp")
    tp = lax.axis_index("tp")
    chip, core = tp // 2, tp % 2
    quarter_x = (dp + 2) % 4
    quarter_y = dp + 1 - 2 * (dp % 2)
    quarter_d = (quarter_x + 1) - 2 * (quarter_x % 2)
    at_x, at_y = (quarter_x, tp), (quarter_y, tp)
    at_up, at_down, at_core = (dp, tp + 2), (dp, tp - 2), (dp, tp + 1 - 2 * core)
    has_up, has_down = chip < N_CHIPS - 1, chip > 0
    own_refs, all_refs = (w_up_ref, w_down_ref, w_out_ref, w_qkv_ref), (up_all, down_all, out_all, qkv_all)
    tok_refs, tok_all = (u_ref, c_ref), (u_all, c_all)
    tile_rows = up_tile.shape[0]
    n_tok = u_ref.shape[0]

    barrier = pltpu.get_barrier_semaphore()
    for target in (at_x, at_y, at_core):
        pl.semaphore_signal(barrier, inc=1, device_id=target, device_id_type=MESH_ID)

    @pl.when(has_up)
    def _():
        pl.semaphore_signal(barrier, inc=1, device_id=at_up, device_id_type=MESH_ID)

    @pl.when(has_down)
    def _():
        pl.semaphore_signal(barrier, inc=1, device_id=at_down, device_id_type=MESH_ID)

    pl.semaphore_wait(barrier, 3 + has_up.astype(jnp.int32) + has_down.astype(jnp.int32))

    def send(kind, arr, src_chip, src, dst, target):
        recv_kind = 0 if kind == 1 else kind
        return pltpu.make_async_remote_copy(
            src_ref=src, dst_ref=dst, send_sem=send_sem.at[kind, arr, src_chip],
            recv_sem=recv_sem.at[recv_kind, arr, src_chip], device_id=target, device_id_type=MESH_ID)

    def line_copy(kind, arr, src_chip, from_own):
        dst = all_refs[arr].at[src_chip, dp]
        src = own_refs[arr].at[dp] if from_own else dst
        return send(kind, arr, src_chip, src, dst, at_up if kind == 0 else at_down)

    def token_copy(kind, i, src_chip, from_own):
        dst = tok_all[i].at[2 * src_chip + core]
        src = tok_refs[i] if from_own else dst
        return send(kind, N_WEIGHTS + i, src_chip, src, dst, (at_up, at_down, at_core)[kind])

    def plane_copy(kind, arr, src_chip):
        rows = all_refs[arr].shape[2]
        half = rows // 2
        if kind == 2:
            ref, target = all_refs[arr].at[src_chip, dp], at_x
        elif kind == 3:
            ref, target = all_refs[arr].at[src_chip, dp], at_y
        elif kind == 4:
            ref, target = all_refs[arr].at[src_chip, quarter_x, pl.ds(0, half)], at_y
        else:
            ref, target = all_refs[arr].at[src_chip, quarter_y, pl.ds(half, half)], at_x
        return send(kind, arr, src_chip, ref, ref, target)

    for arr in range(N_WEIGHTS):
        @pl.when(has_up)
        def _():
            line_copy(0, arr, chip, True).start()

        @pl.when(has_down)
        def _():
            line_copy(1, arr, chip, True).start()

    pair = []
    for i, (src, chip_ref) in enumerate(((u_ref, u_chip), (c_ref, c_chip))):
        copy = pltpu.make_async_remote_copy(
            src_ref=src, dst_ref=chip_ref.at[pl.ds(n_tok, n_tok)], send_sem=pair_send.at[i],
            recv_sem=pair_recv.at[i], device_id=at_core, device_id_type=MESH_ID)
        copy.start()
        keep = pltpu.make_async_copy(src, chip_ref.at[pl.ds(0, n_tok)], own_sem.at[i])
        keep.start()
        store = pltpu.make_async_copy(src, tok_all[i].at[tp], own_sem.at[2 + i])
        store.start()
        pair += [copy, keep, store]
    g_ref[...] = jnp.zeros_like(g_ref)
    du_ref[...] = jnp.zeros_like(du_ref)
    for copy in pair:
        copy.wait()

    def tile_step(src_chip, quarter, own):
        def load(refs, lead):
            return [pltpu.make_async_copy(ref.at[lead + (quarter, pl.ds(0, tile_rows))], buf, tile_sem.at[i])
                    for i, (ref, buf) in enumerate(zip(refs, (up_tile, down_tile)))]

        @pl.when(own)
        def _():
            for copy in load(own_refs, ()):
                copy.start()

        @pl.when(jnp.logical_not(own))
        def _():
            for copy in load(all_refs, (src_chip,)):
                copy.start()

        waits = load(own_refs, ())
        waits[0].wait()
        nt = (((1,), (1,)), ((), ()))
        pre = lax.dot_general(u_chip[...], up_tile[...], nt, preferred_element_type=F32)
        waits[1].wait()
        d_hid = lax.dot_general(c_chip[...], down_tile[...], nt, preferred_element_type=F32)
        hid, pull = jax.vjp(gelu_tanh, pre)
        g_ref[...] += jnp.dot(hid.astype(jnp.bfloat16), down_tile[...], preferred_element_type=F32)
        d_act = pull(d_hid)[0].astype(jnp.bfloat16)
        du_ref[...] += jnp.dot(d_act, up_tile[...], preferred_element_type=F32)

    def hop_chip(hop, side):
        other = chip - hop if side == 0 else chip + hop
        valid = other >= 0 if side == 0 else other < N_CHIPS
        return jnp.clip(other, 0, N_CHIPS - 1), jnp.logical_and(valid, jnp.logical_and(hop >= 1, hop <= N_CHIPS - 1))

    def token_hop(hop):
        for i in range(2):
            for side in range(2):
                other, valid = hop_chip(hop, side)

                @pl.when(valid)
                def _():
                    token_copy(side, i, other, False).wait_recv()
                    token_copy(2, i, other, False).start()

                @pl.when(jnp.logical_and(valid, has_up if side == 0 else has_down))
                def _():
                    token_copy(side, i, other, False).start()

    def step(it, carry):
        for arr in range(N_WEIGHTS):
            for side in range(2):
                other, valid = hop_chip(it, side)

                @pl.when(valid)
                def _():
                    line_copy(side, arr, other, False).wait_recv()
                    plane_copy(2, arr, other).start()
                    plane_copy(3, arr, other).start()

                @pl.when(jnp.logical_and(valid, has_up if side == 0 else has_down))
                def _():
                    line_copy(side, arr, other, False).start()

        @pl.when(it == 2)
        def _():
            for i in range(2):
                @pl.when(has_up)
                def _():
                    token_copy(0, i, chip, True).start()

                @pl.when(has_down)
                def _():
                    token_copy(1, i, chip, True).start()

                token_copy(2, i, chip, True).start()

        @pl.when(it < N_CHIPS + 1)
        def _():
            token_hop(it - 2)

        for arr in range(N_WEIGHTS):
            for side in range(2):
                other, valid = hop_chip(it - 1, side)

                @pl.when(valid)
                def _():
                    plane_copy(2, arr, other).wait_recv()
                    plane_copy(4, arr, other).start()
                    plane_copy(3, arr, other).wait_recv()
                    plane_copy(5, arr, other).start()

        for side in range(2):
            other, valid = hop_chip(it - 3, side)

            @pl.when(valid)
            def _():
                for arr in range(N_WEIGHTS):
                    plane_copy(4, arr, other).wait_recv()
                    plane_copy(5, arr, other).wait_recv()

        def tiles(j, carry2):
            side = j // 4
            k = j % 4
            hop = jnp.where(it == 0, 0, jnp.where(k == 3, it - 3, it - 1))
            other = jnp.where(side == 0, chip - hop, chip + hop)
            in_line = jnp.logical_and(other >= 0, other < N_CHIPS)
            foreign = jnp.logical_and(in_line, jnp.logical_and(hop >= 1, hop <= N_CHIPS - 1))
            own = it == 0
            valid = jnp.where(own, side == 0, foreign)
            quarter = jnp.where(k == 0, dp, jnp.where(k == 1, quarter_x, jnp.where(k == 2, quarter_y, quarter_d)))

            @pl.when(valid)
            def _():
                tile_step(jnp.clip(other, 0, N_CHIPS - 1), quarter, own)

            return carry2

        return lax.fori_loop(0, 8, tiles, carry)

    lax.fori_loop(0, N_CHIPS + 3, step, 0)
    token_hop(jnp.int32(N_CHIPS - 1))

    for arr in range(N_WEIGHTS):
        def drain(src_chip, carry):
            @pl.when(jnp.logical_and(has_up, src_chip <= chip))
            def _():
                line_copy(0, arr, src_chip, False).wait_send()

            @pl.when(jnp.logical_and(has_down, src_chip >= chip))
            def _():
                line_copy(1, arr, src_chip, False).wait_send()

            @pl.when(src_chip != chip)
            def _():
                for kind in (2, 3, 4, 5):
                    plane_copy(kind, arr, src_chip).wait_send()

            return carry

        lax.fori_loop(0, N_CHIPS, drain, 0)

    for i in range(2):
        def drain_tokens(src_chip, carry):
            @pl.when(jnp.logical_and(has_up, src_chip <= chip))
            def _():
                token_copy(0, i, src_chip, False).wait_send()

            @pl.when(jnp.logical_and(has_down, src_chip >= chip))
            def _():
                token_copy(1, i, src_chip, False).wait_send()

            token_copy(2, i, src_chip, False).wait()
            return carry

        lax.fori_loop(0, N_CHIPS, drain_tokens, 0)


def mlp_gather(u_own, c_own, *weight_rows):
    n_tok, width = u_own.shape
    tile_rows = weight_rows[0].shape[1]
    acc = jax.ShapeDtypeStruct((2 * n_tok, width), F32)
    gathered = [jax.ShapeDtypeStruct((N_CHIPS,) + r.shape, r.dtype) for r in weight_rows]
    gathered += [jax.ShapeDtypeStruct((2 * N_CHIPS,) + u_own.shape, u_own.dtype)] * 2
    vmem, anywhere = pl.BlockSpec(memory_space=pltpu.VMEM), pl.BlockSpec(memory_space=pl.ANY)
    n_col = N_CHIPS * 4 * tile_rows
    return pl.pallas_call(
        mlp_kernel,
        out_shape=[acc, acc] + gathered,
        in_specs=[vmem, vmem] + [anywhere] * N_WEIGHTS,
        out_specs=[vmem, vmem] + [anywhere] * (N_WEIGHTS + 2),
        scratch_shapes=[
            pltpu.VMEM((2 * n_tok, width), jnp.bfloat16),
            pltpu.VMEM((2 * n_tok, width), jnp.bfloat16),
            pltpu.VMEM((tile_rows, width), jnp.bfloat16),
            pltpu.VMEM((tile_rows, width), jnp.bfloat16),
            pltpu.SemaphoreType.DMA((2,)),
            pltpu.SemaphoreType.DMA((2,)),
            pltpu.SemaphoreType.DMA((2,)),
            pltpu.SemaphoreType.DMA((4,)),
            pltpu.SemaphoreType.DMA((6, N_WEIGHTS + 2, N_CHIPS)),
            pltpu.SemaphoreType.DMA((6, N_WEIGHTS + 2, N_CHIPS)),
        ],
        compiler_params=pltpu.CompilerParams(collective_id=0, has_side_effects=True, vmem_limit_bytes=48 * 1024 * 1024),
        cost_estimate=pl.CostEstimate(flops=8 * 2 * n_tok * width * n_col * 4, bytes_accessed=64 * 1024 * 1024, transcendentals=0),
        name="mlp_gather",
    )(u_own, c_own, *weight_rows)


def local_backward(y_one, y_two, dy_one, dy_two, w_qkv, w_out, w_up, w_down):
    attn_scale = w_qkv.shape[4] ** -0.5
    wq_layer, wo_layer, wu_layer, wd_layer = w_qkv[0], w_out[0], w_up[0], w_down[0]
    n_seq, n_pos, width = y_one.shape
    n_tok = n_seq * n_pos
    n_heads, head_dim = wo_layer.shape[0], wo_layer.shape[1]
    wo_flat = wo_layer.reshape(n_heads * head_dim, width)
    dp_idx = lax.axis_index("dp")
    tp_idx = lax.axis_index("tp")
    chip = tp_idx // 2
    f_loc = wu_layer.shape[1]
    f_quarter, o_quarter = f_loc // 4, n_heads * head_dim // 4

    u_own = rms_norm(y_one).astype(jnp.bfloat16)
    c_own = dy_two.astype(jnp.bfloat16)
    wqkv_rows = wq_layer.reshape(width, 3 * n_heads * head_dim).T
    own_rows = [w.reshape(4, w.shape[0] // 4, width) for w in (wu_layer.T, wd_layer, wo_flat, wqkv_rows)]
    g_sum, du_sum, _, _, out_all, qkv_rows_all, u_mlp, cot_mlp = mlp_gather(u_own.reshape(n_tok, width), c_own.reshape(n_tok, width), *own_rows)
    g_own = g_sum[:n_tok] + swap_core(g_sum[n_tok:])
    du_own = du_sum[:n_tok] + swap_core(du_sum[n_tok:])
    core_out = lax.dynamic_update_index_in_dim(out_all, own_rows[2], chip, 0).reshape(N_CHIPS, n_heads * head_dim, width)
    core_qkv = lax.dynamic_update_index_in_dim(qkv_rows_all, own_rows[3], chip, 0).reshape(N_CHIPS, 3 * n_heads * head_dim, width)
    other_out, other_qkv = swap_core(core_out), swap_core(core_qkv)
    x_two = y_two - g_own.reshape(y_two.shape)
    dy_one = dy_one + rms_back(y_one, du_own.reshape(y_one.shape))

    u_mlp = u_mlp.reshape(2 * N_CHIPS * n_tok, width)
    cot_mlp = cot_mlp.reshape(2 * N_CHIPS * n_tok, width)
    hidden, gelu_pull = jax.vjp(gelu_tanh, dot(u_mlp, wu_layer, 1, 0))
    hidden_b = hidden.astype(jnp.bfloat16)
    grad_down = dot(hidden_b, cot_mlp, 0, 0)
    d_pre = gelu_pull(dot(cot_mlp, wd_layer, 1, 1))[0].astype(jnp.bfloat16)
    grad_up = dot(u_mlp, d_pre, 0, 0)

    u_att = gather_positions(rms_norm(x_two).astype(jnp.bfloat16))
    cut = n_seq - n_seq // 4
    halves = (slice(0, cut), slice(cut, n_seq))
    c_att = dy_one.astype(jnp.bfloat16)
    c_att, u_att, grad_up, grad_down = lax.optimization_barrier((c_att, u_att, grad_up, grad_down))
    cot_halves = [gather_positions(c_att[rows]) for rows in halves]
    qkv_all = jnp.einsum("bsh,hnjd->jbnsd", u_att, wq_layer, preferred_element_type=F32).astype(jnp.bfloat16)
    q_heads, k_heads, v_heads = qkv_all[0], qkv_all[1], qkv_all[2]
    scores = jnp.einsum("bnqd,bnkd->bnqk", q_heads, k_heads, preferred_element_type=F32) * attn_scale
    attn_prob = jax.nn.softmax(scores, axis=-1)
    prob_b = attn_prob.astype(jnp.bfloat16)
    context = jnp.einsum("bnqk,bnkd->bnqd", prob_b, v_heads, preferred_element_type=F32).astype(jnp.bfloat16)

    core = tp_idx % 2

    def to_positions(by_pos):
        n_b, n_k = by_pos.shape[1], by_pos.shape[2]
        return lax.all_to_all(by_pos.reshape(2 * N_CHIPS, n_pos * n_b, n_k), "tp", 0, 0).reshape(N_CHIPS, 2, n_pos * n_b, n_k)

    def sum_heads(recv, core_rows, other_rows):
        total = jnp.zeros((recv.shape[2], width), F32)
        for which, rows in ((core, core_rows), (1 - core, other_rows)):
            total = total + jnp.einsum("ztk,zkh->th", lax.dynamic_index_in_dim(recv, which, 1, keepdims=False), rows, preferred_element_type=F32)
        return total.reshape(n_pos, -1, width).transpose(1, 0, 2)

    ctx_pos = context.transpose(2, 0, 1, 3).reshape(2 * N_CHIPS * n_pos, n_seq, n_heads * head_dim)
    x_one = y_one - sum_heads(to_positions(ctx_pos), core_out, other_out)

    du_parts, grad_qkv, grad_out = [], None, None
    for part_idx, rows in enumerate(halves):
        cot_half = cot_halves[part_idx]
        prob, prob_half = attn_prob[rows], prob_b[rows]
        d_context = jnp.einsum("bqh,ndh->bnqd", cot_half, wo_layer, preferred_element_type=F32).astype(jnp.bfloat16)
        d_prob = jnp.einsum("bnqd,bnkd->bnqk", d_context, v_heads[rows], preferred_element_type=F32)
        d_value = jnp.einsum("bnqk,bnqd->bnkd", prob_half, d_context, preferred_element_type=F32)
        d_scores = (prob * (d_prob - jnp.sum(d_prob * prob, axis=-1, keepdims=True)) * attn_scale).astype(jnp.bfloat16)
        d_query = jnp.einsum("bnqk,bnkd->bnqd", d_scores, k_heads[rows], preferred_element_type=F32)
        d_key = jnp.einsum("bnqk,bnqd->bnkd", d_scores, q_heads[rows], preferred_element_type=F32)
        d_qkv = jnp.stack([d_query.astype(jnp.bfloat16), d_key.astype(jnp.bfloat16), d_value.astype(jnp.bfloat16)])
        d_pos = d_qkv.transpose(3, 1, 2, 0, 4).reshape(2 * N_CHIPS * n_pos, cot_half.shape[0], 3 * n_heads * head_dim)
        if part_idx == 1:
            d_pos, du_parts[0] = lax.optimization_barrier((d_pos, du_parts[0]))
        du_parts.append(to_positions(d_pos))
        grad_qkv_part = jnp.einsum("bsh,jbnsd->hnjd", u_att[rows], d_qkv, preferred_element_type=F32)
        grad_out_part = jnp.einsum("bnqd,bqh->ndh", context[rows], cot_half, preferred_element_type=F32)
        if part_idx == 0:
            cot_halves[1], grad_qkv, grad_out = lax.optimization_barrier((cot_halves[1], grad_qkv_part, grad_out_part))
        else:
            grad_qkv, grad_out = grad_qkv + grad_qkv_part, grad_out + grad_out_part
    du_att = [sum_heads(recv, core_qkv, other_qkv) for recv in du_parts]
    dx_two = dy_two + rms_back(x_two, jnp.concatenate(du_att, axis=0))
    return (x_one, x_two, dy_one, dx_two, grad_qkv[None], grad_out[None], grad_up[None], grad_down[None])


def solution(mesh):
    state_spec = P("dp", "tp", None)
    in_specs = (state_spec, state_spec, state_spec, state_spec, P(None, None, "tp", None, None), P(None, "tp", None, None), P(None, None, "tp"), P(None, "tp", None))
    out_specs = (state_spec, state_spec, state_spec, state_spec, P("dp", None, "tp", None, None), P("dp", "tp", None, None), P("dp", None, "tp"), P("dp", "tp", None))
    return jax.shard_map(local_backward, mesh=mesh, in_specs=in_specs, out_specs=out_specs, check_vma=False)
```
